32 devices in a mesh: rows: 8 (over z, x), cols: 4 (over y, core).
Axes of the slice: x: 2, y: 2, z: 4, core: 2. Of those that a mesh axis runs over, the one named last changes fastest.
Arguments:
- bag_index: int32 [512, 128], P(('rows', 'cols')), may hold values from 0 to 262143, as said below
- bag_length: int32 [512, 4], P(('rows', 'cols')), may hold values from 1 to 32
- emb_tables: float32 [4, 262144, 128], P(None, ('rows', 'cols')), may hold values from -0.6 to 0.6
- dense_feats: float32 [512, 128], P(('rows', 'cols')), may hold values from -6 to 6
- w_dense: float32 [128, 1024], replicated, may hold values from -0.5 to 0.5
- w_pair: float32 [10, 1024], replicated, may hold values from -0.5 to 0.5
- top_bias: float32 [1024], replicated, may hold values from -3 to 3
Outputs:
- pooled: float32 [512, 4, 128], P(('rows', 'cols'))
- top_hidden: float32 [512, 1024], P(('rows', 'cols'))
The draws below stay inside these ranges and needn't reach their ends.
Inputs may be any that keep to these rules, and one draw needn't show every extreme that they name: `bag_length`: slots at or past a bag's length are ignored, whatever they hold. `bag_index`: device d holds rows d * 8192 to (d + 1) * 8192 - 1 of every table; among the 2048 slots (live or not) of the samples of one device, at most 128 hold rows of any one device, and in every draw some device's rows receive exactly 128 slots from every device.
All inputs are finite; a program needn't handle non-finite values.
Results may differ from the reference program's by a relative error of at most 0.0001.
Values sent between devices are 32-bit elements; how exact they have to be, the bound alone decides.
A program may use at most 128 MiB of HBM per device.

```python
import jax
import jax.numpy as jnp
from jax import lax

E = 128
ROWS_DEV = 8192
NT = 4
L = 32
H = 1024
SAMP_DEV = 16
B = 512
VOCAB = 262144
PAIRS = 10


def draw_bag_index(key, part):
    ndevices = B // SAMP_DEV
    slots = SAMP_DEV * NT * L
    capacity = 2 * slots // ndevices
    total = ndevices * capacity
    token_owner = jnp.arange(total, dtype=jnp.int32) // capacity
    key_weight, key_common, key_blocks = jax.random.split(key, 3)
    weight = jax.random.randint(key_weight, (ndevices,), 0, 4, dtype=jnp.int32) * 512
    common_hot = jax.random.randint(key_common, (), 0, ndevices, dtype=jnp.int32)

    def one_block(block_key):
        key_own, key_score, key_order, key_first, key_second = jax.random.split(block_key, 5)
        own_hot = jax.random.randint(key_own, (), 0, ndevices, dtype=jnp.int32)
        forced = jnp.where((token_owner == common_hot) | (token_owner == own_hot), 4096, 0).astype(jnp.int32)
        score = jax.random.randint(key_score, (total,), 0, 1024, dtype=jnp.int32) + weight[token_owner] + forced
        score = score * total + jnp.arange(total, dtype=jnp.int32)
        unused, chosen = lax.top_k(score, slots)
        order = jax.random.permutation(key_order, slots)
        owners = token_owner[chosen[order]]
        first_draw = jax.random.randint(key_first, (slots,), 0, ROWS_DEV, dtype=jnp.int32)
        second_draw = jax.random.randint(key_second, (slots,), 1, ROWS_DEV + 1, dtype=jnp.int32)
        local = first_draw * second_draw // ROWS_DEV
        return (owners * ROWS_DEV + local).reshape(SAMP_DEV, NT * L)
    block_keys = jax.random.split(key_blocks, ndevices)
    return jax.vmap(one_block)(block_keys).reshape(B, NT * L).astype(jnp.int32)


def touch_ends(drawn, own_key, least, largest):
    dims = drawn.shape
    spot = [jax.random.randint(jax.random.fold_in(own_key, axis), (), 0, dims[axis]) for axis in range(len(dims))]
    drawn = drawn.at[tuple(spot)].set(least)
    longest = dims.index(max(dims))
    spot[longest] = (spot[longest] + 1) % dims[longest]
    return drawn.at[tuple(spot)].set(largest)


def block_scale(own_key, extent, cuts, smallest, largest):
    factor_of = 1.0
    for axis_at, parts in cuts:
        draws = jax.random.uniform(jax.random.fold_in(jax.random.fold_in(own_key, 6), axis_at), (parts,), jnp.float32, smallest / len(cuts), largest / len(cuts))
        factor_of = factor_of * jnp.repeat(jnp.exp(draws), extent[axis_at] // parts).reshape((-1,) + (1,) * (len(extent) - 1 - axis_at))
    return factor_of


def normal_values(stream_key, shape, spread, bound, cuts=(), held_as=jnp.bfloat16):
    drawn = spread * jax.random.normal(stream_key, shape, jnp.float32)
    if cuts:
        drawn = drawn * block_scale(stream_key, shape, cuts, -0.22, 0.18)
    return jnp.clip(drawn, -bound, bound).astype(held_as)


def setup_inputs(seed: int = 0) -> dict:
    seeds = jax.random.split(jax.random.key(seed), 8)
    return {
        "bag_index": draw_bag_index(jax.random.fold_in(seeds[7], 71), 0),
        "bag_length": touch_ends(jax.random.randint(seeds[1], (B, NT), 1, L + 1), jax.random.fold_in(seeds[1], 1), 1, L).astype(jnp.int32),
        "emb_tables": normal_values(seeds[2], (NT, VOCAB, E), 0.1, 0.6, ((1, 32),), jnp.float32),
        "dense_feats": normal_values(seeds[3], (B, E), 1.0, 6.0, ((0, 32),), jnp.float32),
        "w_dense": normal_values(seeds[4], (E, H), (E + PAIRS) ** -0.5, 0.5, (), jnp.float32),
        "w_pair": normal_values(seeds[5], (PAIRS, H), (E + PAIRS) ** -0.5, 0.5, (), jnp.float32),
        "top_bias": normal_values(seeds[6], (H,), 0.5, 3.0, (), jnp.float32),
    }


def interact(dense_feats, pooled, w_dense, w_pair, top_bias):
    feats = [dense_feats] + [pooled[:, t, :] for t in range(NT)]
    pair_list = []
    for first in range(NT + 1):
        for second in range(first + 1, NT + 1):
            pair_list.append(jnp.sum(feats[first] * feats[second], axis=-1))
    pair_dots = jnp.stack(pair_list, axis=1)
    hidden = jnp.dot(dense_feats, w_dense, precision=lax.Precision.HIGHEST, preferred_element_type=jnp.float32)
    hidden = hidden + jnp.dot(pair_dots, w_pair, precision=lax.Precision.HIGHEST, preferred_element_type=jnp.float32)
    return jnp.maximum(hidden + top_bias, 0.0)


def reference(bag_index, bag_length, emb_tables, dense_feats, w_dense, w_pair, top_bias):
    position = jnp.arange(L, dtype=jnp.int32)
    pieces = []
    for table in range(NT):
        ids = bag_index[:, table * L:(table + 1) * L]
        live = position[None, :] < bag_length[:, table:table + 1]
        picked = jnp.take(emb_tables[table], ids, axis=0)
        pieces.append(jnp.sum(jnp.where(live[:, :, None], picked, 0.0), axis=1))
    pooled = jnp.stack(pieces, axis=1)
    return pooled, interact(dense_feats, pooled, w_dense, w_pair, top_bias)
```

```python
import functools

import jax
import jax.numpy as jnp
from jax import lax
from jax.experimental import pallas as pl
from jax.experimental.pallas import tpu as pltpu
from jax.sharding import PartitionSpec as P

LOGICAL = pl.DeviceIdType.LOGICAL
F32 = jnp.float32
BF16 = jnp.bfloat16
LAG = 5
CHUNKS = 8


def kernel(
    dims,
    index_hbm,
    length_hbm,
    table_hbm,
    dense_hbm,
    wd_hbm,
    wp_hbm,
    bias_hbm,
    pooled_ref,
    hidden_ref,
    index_ref,
    length_ref,
    table,
    dense_ref,
    wd,
    wp_ref,
    bias_ref,
    row_out,
    bag_out,
    bag_in,
    ids,
    rows_a,
    rows_b,
    rows_c,
    rows_d,
    core_out,
    core_in,
    keep,
    plane_out,
    plane_in,
    z_out,
    z_in,
    load_sem,
    table_sem,
    box_send,
    box_recv,
    core_send,
    core_recv,
    plane_send,
    plane_recv,
    z_send,
    z_recv,
):
    nr, nc, nx, local_rows, nt, slots_bag, cap = dims
    n = nr * nc
    ny = nc // 2
    np_ = nx * ny
    nz = nr // nx
    groups = nz * np_
    samples, lanes = index_ref.shape
    width = table.shape[1]
    bags = samples * nt
    total_rows = nt * local_rows
    r = lax.axis_index("rows")
    c = lax.axis_index("cols")
    z, x, y, k = r // nx, r % nx, c // 2, c % 2

    hops = sorted(
        [(dx, dy) for dx in range(nx) for dy in range(ny)],
        key=lambda h: (-min(h[0], nx - h[0]) - min(h[1], ny - h[1]), h),
    )
    back = [hops.index(((-dx) % nx, (-dy) % ny)) for dx, dy in hops]

    def plane_at(i):
        if i == nz - 1:
            return z
        low = jnp.where(nz - 1 - i > z, nz - 1 - i, nz - 2 - i)
        high = jnp.where(i < z, i, i + 1)
        return jnp.where(2 * z < nz, low, high)

    def turn_at(zz):
        low = jnp.where(z > zz, nz - 1 - z, nz - 2 - z)
        high = jnp.where(z < zz, z, z - 1)
        return jnp.where(2 * zz < nz, low, high)

    planes = [plane_at(i) for i in range(nz)]
    turns = [turn_at(planes[i]) for i in range(nz - 1)] + [nz - 1]
    chips = [(((x + dx) % nx), ((y + dy) % ny)) for dx, dy in hops]

    def flat(zz, chip, kk):
        return (zz * nx + chip[0]) * nc + chip[1] * 2 + kk

    peers = []
    for i in range(nz):
        for q in range(np_):
            for same in range(2):
                if (i, q, same) != (nz - 1, np_ - 1, 1):
                    d = flat(planes[i], chips[q], k if same else 1 - k)
                    peers.append((d, (turns[i] * np_ + back[q]) * 2 + same))
    own_slot = n - 1

    load = lambda i, source, target: pltpu.make_async_copy(source, target, load_sem.at[i])
    index_copy = load(0, index_hbm, index_ref)
    length_copy = load(1, length_hbm, length_ref)
    wd_copy = load(2, wd_hbm, wd)
    dense_copy = load(3, dense_hbm, dense_ref)
    wp_copy = load(4, wp_hbm, wp_ref)
    bias_copy = load(5, bias_hbm, bias_ref)
    index_copy.start()
    length_copy.start()
    barrier = pltpu.get_barrier_semaphore()
    for d, slot in peers:
        pl.semaphore_signal(barrier, inc=1, device_id=d, device_id_type=LOGICAL)
    wd_copy.start()
    dense_copy.start()
    bias_copy.start()
    wp_copy.start()
    part = total_rows // CHUNKS
    for i in range(CHUNKS):
        rows = pl.ds(i * part, part)
        pltpu.make_async_copy(table_hbm.at[rows], table.at[rows], table_sem).start()

    index_copy.wait()
    length_copy.wait()
    idx = index_ref[...]
    lane = lax.broadcasted_iota(jnp.int32, (samples, lanes), 1)
    table_of = lane // slots_bag
    length = length_ref[...].astype(F32)
    diagonal = (
        lax.broadcasted_iota(jnp.int32, (samples, samples), 0)
        == lax.broadcasted_iota(jnp.int32, (samples, samples), 1)
    )
    lengths = jnp.zeros((samples, lanes), F32)
    for t in range(nt):
        column = jnp.sum(jnp.where(diagonal, length[t : t + 1, :], 0.0), axis=1, keepdims=True)
        lengths = jnp.where(table_of == t, column, lengths)
    live = lane - table_of * slots_bag < lengths.astype(jnp.int32)
    if local_rows & (local_rows - 1) == 0:
        owner = lax.shift_right_logical(idx, jnp.full_like(idx, local_rows.bit_length() - 1))
    else:
        owner = idx // local_rows
    row = table_of * local_rows + idx - owner * local_rows
    bag = lax.broadcasted_iota(jnp.int32, (samples, lanes), 0) * nt + table_of
    owner = jnp.where(live, owner, -1)
    pieces = []
    shift = 0
    while shift == 0 or (total_rows - 1) >> shift:
        pieces.append((row // (1 << shift)) % 256)
        shift += 8
    n_row = len(pieces)
    shift = 0
    while shift == 0 or bags >> shift:
        pieces.append(((bag + 1) // (1 << shift)) % 256)
        shift += 8
    pieces = [v.astype(F32) for v in pieces]
    dev_iota = lax.broadcasted_iota(jnp.int32, (n, lanes), 0)
    before = (
        lax.broadcasted_iota(jnp.int32, (lanes, lanes), 0)
        < lax.broadcasted_iota(jnp.int32, (lanes, lanes), 1)
    )
    before = jnp.where(before, 1.0, 0.0).astype(BF16)
    hots = [
        jnp.where(owner[b : b + 1, :] == dev_iota, 1.0, 0.0).astype(F32) for b in range(samples)
    ]
    prefix = jnp.dot(
        jnp.concatenate([h.astype(BF16) for h in hots], axis=0), before, preferred_element_type=F32
    )
    base = jnp.zeros((n, 1), F32)
    box = jnp.zeros((len(pieces) * n, cap), F32)
    cap_iota = lax.broadcasted_iota(jnp.int32, (cap, lanes), 0)
    for b in range(samples):
        hot = hots[b]
        rank = jnp.sum(hot * (prefix[b * n : (b + 1) * n, :] + base), axis=0, keepdims=True)
        base = base + jnp.sum(hot, axis=1, keepdims=True)
        spot = jnp.where(rank.astype(jnp.int32) == cap_iota, 1.0, 0.0).astype(BF16)
        coded = jnp.concatenate([hot * v[b : b + 1, :] for v in pieces], axis=0).astype(BF16)
        box = box + lax.dot_general(
            coded, spot, (((1,), (1,)), ((), ())), preferred_element_type=F32
        )
    box_row = jnp.zeros((n, cap), jnp.int32)
    box_bag = jnp.full((n, cap), -1, jnp.int32)
    for i in range(len(pieces)):
        piece = box[i * n : (i + 1) * n, :].astype(jnp.int32)
        if i < n_row:
            box_row = box_row + piece * (1 << (8 * i))
        else:
            box_bag = box_bag + piece * (1 << (8 * (i - n_row)))
    if total_rows & (total_rows - 1) == 0:
        box_row = box_row & (total_rows - 1)
    else:
        box_row = jnp.clip(box_row, 0, total_rows - 1)
    for d in range(n):
        row_out[d] = box_row[d : d + 1, :]
        bag_out[d] = box_bag[d : d + 1, :]

    pl.semaphore_wait(barrier, n - 1)

    def box_copy(source, target, which, d, slot):
        return pltpu.make_async_remote_copy(
            src_ref=source.at[d],
            dst_ref=target.at[slot],
            send_sem=box_send.at[which],
            recv_sem=box_recv.at[which],
            device_id=d,
            device_id_type=LOGICAL,
        )

    for d, slot in peers:
        box_copy(row_out, ids, 0, d, slot).start()
    for d, slot in peers:
        box_copy(bag_out, bag_in, 1, d, slot).start()
    me = r * nc + c
    own_ids = load(0, row_out.at[me], ids.at[own_slot])
    own_ids.start()
    bag_in[own_slot] = bag_out[me]

    wd_copy.wait()
    dense_copy.wait()
    bias_copy.wait()
    wp_copy.wait()
    dense = dense_ref[...]
    hidden_ref[...] = (
        jnp.dot(dense, wd[...], precision=lax.Precision.HIGHEST, preferred_element_type=F32)
        + bias_ref[...]
    )

    own_ids.wait()
    pltpu.make_async_copy(table_hbm, table, table_sem).wait()
    others = pl.ds(0, n - 1)
    for which, (source, target) in enumerate(((row_out, ids), (bag_out, bag_in))):
        pltpu.make_async_remote_copy(
            src_ref=source.at[others],
            dst_ref=target.at[others],
            send_sem=box_send.at[which],
            recv_sem=box_recv.at[which],
            device_id=me,
            device_id_type=LOGICAL,
        ).wait_recv()

    bag_iota = lax.broadcasted_iota(jnp.int32, (bags, cap), 0)
    buffers = ((rows_a, rows_b), (rows_c, rows_d))

    def fetch(slot, target):
        for i in range(cap):
            target[i : i + 1, :] = table[pl.ds(ids[slot, 0, i], 1), :]

    def pool(slot, source):
        found = source[...]
        high = found.astype(BF16)
        low = (found - high.astype(F32)).astype(BF16)
        select = jnp.where(bag_in[slot] == bag_iota, 1.0, 0.0).astype(BF16)
        both = jnp.dot(select, jnp.concatenate([high, low], axis=1), preferred_element_type=F32)
        return both[:, :width] + both[:, width:]

    def copy(source, target, send, recv, d):
        return pltpu.make_async_remote_copy(
            src_ref=source,
            dst_ref=target,
            send_sem=send,
            recv_sem=recv,
            device_id=d,
            device_id_type=LOGICAL,
        )

    mate = flat(z, (x, y), 1 - k)

    def core_copy(j):
        return copy(core_out.at[j], core_in.at[j], core_send, core_recv.at[j], mate)

    def forward(j):
        i, q = j // np_, j % np_
        core_copy(j).wait_recv()
        summed = core_in[j] + keep[j]
        if q == np_ - 1:
            keep[j] = summed
        else:
            at = i * (np_ - 1) + q
            to = i * (np_ - 1) + back[q]
            plane_out[at] = summed
            copy(
                plane_out.at[at],
                plane_in.at[to],
                plane_send,
                plane_recv.at[i],
                flat(z, chips[q], k),
            ).start()

    def collect(i):
        some = pl.ds(i * (np_ - 1), np_ - 1)
        copy(plane_out.at[some], plane_in.at[some], plane_send, plane_recv.at[i], me).wait_recv()
        summed = keep[i * np_ + np_ - 1]
        for q in range(np_ - 1):
            summed = summed + plane_in[i * (np_ - 1) + q]
        if i < nz - 1:
            z_out[i] = summed
            copy(
                z_out.at[i], z_in.at[turns[i]], z_send, z_recv, flat(planes[i], (x, y), k)
            ).start()
        return summed

    for j in range(groups + 1):
        if j < groups:
            fetch(2 * j, buffers[j % 2][0])
            fetch(2 * j + 1, buffers[j % 2][1])
        if j > 0:
            core_out[j - 1] = pool(2 * j - 2, buffers[(j - 1) % 2][0])
            keep[j - 1] = pool(2 * j - 1, buffers[(j - 1) % 2][1])
            core_copy(j - 1).start()
        if j >= LAG:
            forward(j - LAG)
    for j in range(groups + 1 - LAG, groups):
        forward(j)
    for i in range(nz):
        pooled = collect(i)
    if nz > 1:
        copy(z_out, z_in, z_send, z_recv, me).wait_recv()
        for i in range(nz - 1):
            pooled = pooled + z_in[i]

    pooled_ref[...] = pooled
    feats = [dense] + [pooled_ref[pl.ds(t, samples, stride=nt), :] for t in range(nt)]
    total = hidden_ref[...]
    pair = 0
    for first in range(nt + 1):
        for second in range(first + 1, nt + 1):
            dots = jnp.sum(feats[first] * feats[second], axis=-1, keepdims=True)
            total = total + dots * wp_ref[pair : pair + 1, :]
            pair += 1
    hidden_ref[...] = total

    for which, (source, target) in enumerate(((row_out, ids), (bag_out, bag_in))):
        pltpu.make_async_remote_copy(
            src_ref=source.at[others],
            dst_ref=target.at[others],
            send_sem=box_send.at[which],
            recv_sem=box_recv.at[which],
            device_id=me,
            device_id_type=LOGICAL,
        ).wait_send()
    copy(core_out, core_in, core_send, core_recv.at[0], me).wait_send()
    if np_ > 1:
        copy(plane_out, plane_in, plane_send, plane_recv.at[0], me).wait_send()
    if nz > 1:
        copy(z_out, z_in, z_send, z_recv, me).wait_send()


def finish(pooled_ref, total_ref, pooled_out, hidden_out):
    pooled_out[...] = pooled_ref[...]
    hidden_out[...] = jnp.maximum(total_ref[...], 0.0)


def shards(nr, nc, bag_index, bag_length, emb_tables, dense_feats, w_dense, w_pair, top_bias):
    samples, lanes = bag_index.shape
    nt, local_rows, width = emb_tables.shape
    n = nr * nc
    slots = samples * lanes
    cap = 2 * slots // n
    bags = samples * nt
    units = w_dense.shape[1]
    nx = 2 if nr % 2 == 0 else 1
    groups = n // 2
    nz = nr // nx
    np_ = groups // nz
    dims = (nr, nc, nx, local_rows, nt, lanes // nt, cap)
    vmem = pl.BlockSpec(memory_space=pltpu.VMEM)
    hbm = pl.BlockSpec(memory_space=pltpu.HBM)
    blocks = lambda m: pltpu.VMEM((max(m, 1), bags, width), F32)
    dma = pltpu.SemaphoreType.DMA
    results = (
        jax.ShapeDtypeStruct((bags, width), F32),
        jax.ShapeDtypeStruct((samples, units), F32),
    )
    total_rows = nt * local_rows
    pooled, total = pl.pallas_call(
        functools.partial(kernel, dims),
        out_shape=(pltpu.VMEM((bags, width), F32), pltpu.VMEM((samples, units), F32)),
        in_specs=[hbm] * 7,
        out_specs=(vmem, vmem),
        scratch_shapes=[
            pltpu.VMEM((samples, lanes), jnp.int32),
            pltpu.VMEM((nt, samples), jnp.int32),
            pltpu.VMEM((total_rows, width), F32),
            pltpu.VMEM((samples, width), F32),
            pltpu.VMEM(w_dense.shape, F32),
            pltpu.VMEM(w_pair.shape, F32),
            pltpu.VMEM((1, units), F32),
            pltpu.VMEM((n, 1, cap), jnp.int32),
            pltpu.VMEM((n, 1, cap), jnp.int32),
            pltpu.VMEM((n, 1, cap), jnp.int32),
            pltpu.SMEM((n, 1, cap), jnp.int32),
            pltpu.VMEM((cap, width), F32),
            pltpu.VMEM((cap, width), F32),
            pltpu.VMEM((cap, width), F32),
            pltpu.VMEM((cap, width), F32),
            blocks(groups),
            blocks(groups),
            blocks(groups),
            blocks(nz * (np_ - 1)),
            blocks(nz * (np_ - 1)),
            blocks(nz - 1),
            blocks(nz - 1),
            dma((6,)),
            dma,
            dma((2,)),
            dma((2,)),
            dma,
            dma((groups,)),
            dma,
            dma((nz,)),
            dma,
            dma,
        ],
        compiler_params=pltpu.CompilerParams(
            collective_id=0, has_side_effects=True, vmem_limit_bytes=64000 * 1024
        ),
    )(
        bag_index,
        bag_length.T,
        emb_tables.reshape(total_rows, width),
        dense_feats,
        w_dense,
        w_pair,
        top_bias.reshape(1, units),
    )
    pooled, hidden = pl.pallas_call(
        finish,
        out_shape=results,
        in_specs=[vmem, vmem],
        out_specs=(vmem, vmem),
        compiler_params=pltpu.CompilerParams(vmem_limit_bytes=4 * 1024 * 1024),
    )(pooled, total)
    return pooled.reshape(samples, nt, width), hidden


def solution(mesh):
    nr, nc = mesh.shape["rows"], mesh.shape["cols"]
    in_specs = (
        P(("rows", "cols"), None),
        P(("rows", "cols"), None),
        P(None, ("rows", "cols"), None),
        P(("rows", "cols"), None),
        P(),
        P(),
        P(),
    )
    out_specs = (P(("rows", "cols"), None, None), P(("rows", "cols"), None))
    return jax.shard_map(
        functools.partial(shards, nr, nc),
        mesh=mesh,
        in_specs=in_specs,
        out_specs=out_specs,
        check_vma=False,
    )
```

```python
import functools

import jax
import jax.numpy as jnp
from jax import lax
from jax.experimental import pallas as pl
from jax.experimental.pallas import tpu as pltpu
from jax.sharding import PartitionSpec as P

LOGICAL = pl.DeviceIdType.LOGICAL
F32 = jnp.float32
BF16 = jnp.bfloat16
LAG = 5
DIRECT = 1
CHUNKS = 8


def near_pairs(nz):
    last = {}
    for z in range(nz):
        turns = [zz for zz in (range(nz - 1, -1, -1) if 2 * z < nz else range(nz)) if zz != z]
        last[z] = turns[-1] if turns else z
    return nz > 1 and all(last[last[z]] == z for z in range(nz))


def kernel(
    dims,
    index_hbm,
    length_hbm,
    table_hbm,
    dense_hbm,
    wd_hbm,
    wp_hbm,
    bias_hbm,
    pooled_ref,
    hidden_ref,
    index_ref,
    length_ref,
    table,
    dense_ref,
    wd,
    wp_ref,
    bias_ref,
    row_out,
    bag_out,
    bag_in,
    ids,
    rows_a,
    rows_b,
    rows_c,
    rows_d,
    core_out,
    core_in,
    keep,
    plane_out,
    plane_in,
    z_out,
    z_in,
    near_out,
    near_in,
    load_sem,
    table_sem,
    box_send,
    box_recv,
    core_send,
    core_recv,
    plane_send,
    plane_recv,
    z_send,
    z_recv,
    near_send,
    near_recv,
):
    nr, nc, nx, local_rows, nt, slots_bag, cap = dims
    n = nr * nc
    ny = nc // 2
    np_ = nx * ny
    around = 2 * np_
    nz = nr // nx
    groups = nz * np_
    samples, lanes = index_ref.shape
    width = table.shape[1]
    bags = samples * nt
    total_rows = nt * local_rows
    r = lax.axis_index("rows")
    c = lax.axis_index("cols")
    z, x, y, k = r // nx, r % nx, c // 2, c % 2

    hops = sorted(
        [(dx, dy) for dx in range(nx) for dy in range(ny)],
        key=lambda h: (-min(h[0], nx - h[0]) - min(h[1], ny - h[1]), h),
    )
    back = [hops.index(((-dx) % nx, (-dy) % ny)) for dx, dy in hops]

    def plane_at(i):
        if i == nz - 1:
            return z
        low = jnp.where(nz - 1 - i > z, nz - 1 - i, nz - 2 - i)
        high = jnp.where(i < z, i, i + 1)
        return jnp.where(2 * z < nz, low, high)

    def turn_at(zz):
        low = jnp.where(z > zz, nz - 1 - z, nz - 2 - z)
        high = jnp.where(z < zz, z, z - 1)
        return jnp.where(2 * zz < nz, low, high)

    planes = [plane_at(i) for i in range(nz)]
    turns = [turn_at(planes[i]) for i in range(nz - 1)] + [nz - 1]
    chips = [(((x + dx) % nx), ((y + dy) % ny)) for dx, dy in hops]

    def flat(zz, chip, kk):
        return (zz * nx + chip[0]) * nc + chip[1] * 2 + kk

    me = flat(z, (x, y), k)
    mate = flat(z, (x, y), 1 - k)
    peers = []
    for i in range(nz):
        for q in range(np_):
            for same in range(2):
                if (i, q, same) != (nz - 1, np_ - 1, 1):
                    d = flat(planes[i], chips[q], k if same else 1 - k)
                    peers.append((d, turns[i], back[q] * 2 + same))

    near = near_pairs(nz)
    load = lambda i, source, target: pltpu.make_async_copy(source, target, load_sem.at[i])
    index_copy = load(0, index_hbm, index_ref)
    length_copy = load(1, length_hbm, length_ref)
    wd_copy = load(2, wd_hbm, wd)
    dense_copy = load(3, dense_hbm, dense_ref)
    wp_copy = load(4, wp_hbm, wp_ref)
    bias_copy = load(5, bias_hbm, bias_ref)
    index_copy.start()
    length_copy.start()
    barrier = pltpu.get_barrier_semaphore()
    for d, turn, slot in peers:
        pl.semaphore_signal(barrier, inc=1, device_id=d, device_id_type=LOGICAL)
    part = total_rows // CHUNKS
    for i in range(CHUNKS):
        rows = pl.ds(i * part, part)
        pltpu.make_async_copy(table_hbm.at[rows], table.at[rows], table_sem).start()
    wd_copy.start()
    dense_copy.start()
    bias_copy.start()
    wp_copy.start()

    index_copy.wait()
    length_copy.wait()
    idx = index_ref[...]
    lane = lax.broadcasted_iota(jnp.int32, (samples, lanes), 1)
    table_of = lane // slots_bag
    length = length_ref[...].astype(F32)
    diagonal = (
        lax.broadcasted_iota(jnp.int32, (samples, samples), 0)
        == lax.broadcasted_iota(jnp.int32, (samples, samples), 1)
    )
    lengths = jnp.zeros((samples, lanes), F32)
    for t in range(nt):
        column = jnp.sum(jnp.where(diagonal, length[t : t + 1, :], 0.0), axis=1, keepdims=True)
        lengths = jnp.where(table_of == t, column, lengths)
    live = lane - table_of * slots_bag < lengths.astype(jnp.int32)
    if local_rows & (local_rows - 1) == 0:
        owner = lax.shift_right_logical(idx, jnp.full_like(idx, local_rows.bit_length() - 1))
    else:
        owner = idx // local_rows
    row = table_of * local_rows + idx - owner * local_rows
    bag = lax.broadcasted_iota(jnp.int32, (samples, lanes), 0) * nt + table_of
    owner = jnp.where(live, owner, -1)
    pieces = []
    shift = 0
    while shift == 0 or (total_rows - 1) >> shift:
        pieces.append((row // (1 << shift)) % 256)
        shift += 8
    n_row = len(pieces)
    shift = 0
    while shift == 0 or bags >> shift:
        pieces.append(((bag + 1) // (1 << shift)) % 256)
        shift += 8
    pieces = [v.astype(F32) for v in pieces]
    dev_iota = lax.broadcasted_iota(jnp.int32, (n, lanes), 0)
    before = (
        lax.broadcasted_iota(jnp.int32, (lanes, lanes), 0)
        < lax.broadcasted_iota(jnp.int32, (lanes, lanes), 1)
    )
    before = jnp.where(before, 1.0, 0.0).astype(BF16)
    hots = [
        jnp.where(owner[b : b + 1, :] == dev_iota, 1.0, 0.0).astype(F32) for b in range(samples)
    ]
    prefix = jnp.dot(
        jnp.concatenate([h.astype(BF16) for h in hots], axis=0), before, preferred_element_type=F32
    )
    base = jnp.zeros((n, 1), F32)
    box = jnp.zeros((len(pieces) * n, cap), F32)
    cap_iota = lax.broadcasted_iota(jnp.int32, (cap, lanes), 0)
    for b in range(samples):
        hot = hots[b]
        rank = jnp.sum(hot * (prefix[b * n : (b + 1) * n, :] + base), axis=0, keepdims=True)
        base = base + jnp.sum(hot, axis=1, keepdims=True)
        spot = jnp.where(rank.astype(jnp.int32) == cap_iota, 1.0, 0.0).astype(BF16)
        coded = jnp.concatenate([hot * v[b : b + 1, :] for v in pieces], axis=0).astype(BF16)
        box = box + lax.dot_general(
            coded, spot, (((1,), (1,)), ((), ())), preferred_element_type=F32
        )
    box_row = jnp.zeros((n, cap), jnp.int32)
    box_bag = jnp.full((n, cap), -1, jnp.int32)
    for i in range(len(pieces)):
        piece = box[i * n : (i + 1) * n, :].astype(jnp.int32)
        if i < n_row:
            box_row = box_row + piece * (1 << (8 * i))
        else:
            box_bag = box_bag + piece * (1 << (8 * (i - n_row)))
    if total_rows & (total_rows - 1) == 0:
        box_row = box_row & (total_rows - 1)
    else:
        box_row = jnp.clip(box_row, 0, total_rows - 1)
    for d in range(n):
        row_out[d] = box_row[d : d + 1, :]
        bag_out[d] = box_bag[d : d + 1, :]

    def copy(source, target, send, recv, d):
        return pltpu.make_async_remote_copy(
            src_ref=source,
            dst_ref=target,
            send_sem=send,
            recv_sem=recv,
            device_id=d,
            device_id_type=LOGICAL,
        )

    pl.semaphore_wait(barrier, n - 1)
    boxes = ((row_out, ids), (bag_out, bag_in))
    for i, (source, target) in enumerate(boxes):
        for d, turn, slot in peers:
            copy(
                source.at[d], target.at[turn, slot], box_send.at[i], box_recv.at[i, turn], d
            ).start()
    own_ids = load(0, row_out.at[me], ids.at[nz - 1, around - 1])
    own_ids.start()
    bag_in[nz - 1, around - 1] = bag_out[me]

    own_ids.wait()
    pltpu.make_async_copy(table_hbm, table, table_sem).wait()
    def boxes_from(i):
        some = pl.ds(0, around - 1 if i == nz - 1 else around)
        for which, (source, target) in enumerate(boxes):
            copy(
                source.at[some], target.at[i, some], box_send.at[which], box_recv.at[which, i], me
            ).wait_recv()

    bag_iota = lax.broadcasted_iota(jnp.int32, (bags, cap), 0)
    buffers = ((rows_a, rows_b), (rows_c, rows_d))

    def fetch(i, slot, target):
        for at in range(cap):
            target[at : at + 1, :] = table[pl.ds(ids[i, slot, 0, at], 1), :]

    def pool(i, slot, source):
        found = source[...]
        high = found.astype(BF16)
        low = (found - high.astype(F32)).astype(BF16)
        select = jnp.where(bag_in[i, slot] == bag_iota, 1.0, 0.0).astype(BF16)
        both = jnp.dot(select, jnp.concatenate([high, low], axis=1), preferred_element_type=F32)
        return both[:, :width] + both[:, width:]

    def core_copy(j):
        return copy(core_out.at[j], core_in.at[j], core_send, core_recv.at[j], mate)

    def forward(j):
        i, q = j // np_, j % np_
        core_copy(j).wait_recv()
        summed = core_in[j] + keep[j]
        if near and i == nz - 2 and q < DIRECT:
            near_out[q] = summed
            copy(
                near_out.at[q], near_in.at[back[q]], near_send, near_recv, flat(planes[i], chips[q], k)
            ).start()
        elif q == np_ - 1:
            keep[j] = summed
        else:
            at, to = i * (np_ - 1) + q, i * (np_ - 1) + back[q]
            plane_out[at] = summed
            copy(
                plane_out.at[at],
                plane_in.at[to],
                plane_send,
                plane_recv.at[i],
                flat(z, chips[q], k),
            ).start()

    def collect(i):
        skip = DIRECT if near and i == nz - 2 else 0
        first = i * (np_ - 1) + skip
        some = pl.ds(first, np_ - 1 - skip)
        copy(plane_out.at[some], plane_in.at[some], plane_send, plane_recv.at[i], me).wait_recv()
        summed = keep[i * np_ + np_ - 1]
        for q in range(skip, np_ - 1):
            summed = summed + plane_in[i * (np_ - 1) + q]
        if i < nz - 1:
            z_out[i] = summed
            copy(
                z_out.at[i], z_in.at[turns[i]], z_send, z_recv, flat(planes[i], (x, y), k)
            ).start()
        return summed

    order = list(range(groups))
    seen = set()
    for step in range(groups + LAG):
        if step < groups:
            i, q = order[step] // np_, order[step] % np_
            if i not in seen:
                seen.add(i)
                boxes_from(i)
            fetch(i, 2 * q, buffers[step % 2][0])
            fetch(i, 2 * q + 1, buffers[step % 2][1])
        if 0 < step <= groups:
            j = order[step - 1]
            i, q = j // np_, j % np_
            core_out[j] = pool(i, 2 * q, buffers[(step - 1) % 2][0])
            keep[j] = pool(i, 2 * q + 1, buffers[(step - 1) % 2][1])
            core_copy(j).start()
        if step >= LAG:
            forward(order[step - LAG])

    for i in range(nz):
        if i == nz - 1:
            wd_copy.wait()
            dense_copy.wait()
            bias_copy.wait()
            wp_copy.wait()
            dense = dense_ref[...]
            hidden_ref[...] = (
                jnp.dot(dense, wd[...], precision=lax.Precision.HIGHEST, preferred_element_type=F32)
                + bias_ref[...]
            )
        pooled = collect(i)
    if near:
        copy(near_out, near_in, near_send, near_recv, me).wait_recv()
        for q in range(DIRECT):
            pooled = pooled + near_in[q]
    if nz > 1:
        copy(z_out, z_in, z_send, z_recv, me).wait_recv()
        for i in range(nz - 1):
            pooled = pooled + z_in[i]

    pooled_ref[...] = pooled
    feats = [dense] + [pooled_ref[pl.ds(t, samples, stride=nt), :] for t in range(nt)]
    total = hidden_ref[...]
    pair = 0
    for first in range(nt + 1):
        for second in range(first + 1, nt + 1):
            dots = jnp.sum(feats[first] * feats[second], axis=-1, keepdims=True)
            total = total + dots * wp_ref[pair : pair + 1, :]
            pair += 1
    hidden_ref[...] = total

    others = pl.ds(0, n - 1)
    for which, (source, target) in enumerate(boxes):
        copy(
            source.at[others], source.at[others], box_send.at[which], box_recv.at[which, 0], me
        ).wait_send()
    copy(core_out, core_in, core_send, core_recv.at[0], me).wait_send()
    whole = pl.ds(0, nz * (np_ - 1) - (DIRECT if near else 0))
    copy(
        plane_out.at[whole], plane_in.at[whole], plane_send, plane_recv.at[0], me
    ).wait_send()
    if nz > 1:
        copy(z_out, z_in, z_send, z_recv, me).wait_send()
    if near:
        copy(near_out, near_in, near_send, near_recv, me).wait_send()


def finish(pooled_ref, total_ref, pooled_out, hidden_out):
    pooled_out[...] = pooled_ref[...]
    hidden_out[...] = jnp.maximum(total_ref[...], 0.0)


def shards(nr, nc, bag_index, bag_length, emb_tables, dense_feats, w_dense, w_pair, top_bias):
    samples, lanes = bag_index.shape
    nt, local_rows, width = emb_tables.shape
    n = nr * nc
    slots = samples * lanes
    cap = 2 * slots // n
    bags = samples * nt
    units = w_dense.shape[1]
    nx = 2 if nr % 2 == 0 else 1
    groups = n // 2
    nz = nr // nx
    np_ = groups // nz
    dims = (nr, nc, nx, local_rows, nt, lanes // nt, cap)
    vmem = pl.BlockSpec(memory_space=pltpu.VMEM)
    hbm = pl.BlockSpec(memory_space=pltpu.HBM)
    blocks = lambda m: pltpu.VMEM((max(m, 1), bags, width), F32)
    dma = pltpu.SemaphoreType.DMA
    results = (
        jax.ShapeDtypeStruct((bags, width), F32),
        jax.ShapeDtypeStruct((samples, units), F32),
    )
    total_rows = nt * local_rows
    pooled, total = pl.pallas_call(
        functools.partial(kernel, dims),
        out_shape=(pltpu.VMEM((bags, width), F32), pltpu.VMEM((samples, units), F32)),
        in_specs=[hbm] * 7,
        out_specs=(vmem, vmem),
        scratch_shapes=[
            pltpu.VMEM((samples, lanes), jnp.int32),
            pltpu.VMEM((nt, samples), jnp.int32),
            pltpu.VMEM((total_rows, width), F32),
            pltpu.VMEM((samples, width), F32),
            pltpu.VMEM(w_dense.shape, F32),
            pltpu.VMEM(w_pair.shape, F32),
            pltpu.VMEM((1, units), F32),
            pltpu.VMEM((n, 1, cap), jnp.int32),
            pltpu.VMEM((n, 1, cap), jnp.int32),
            pltpu.VMEM((nz, 2 * np_, 1, cap), jnp.int32),
            pltpu.SMEM((nz, 2 * np_, 1, cap), jnp.int32),
            pltpu.VMEM((cap, width), F32),
            pltpu.VMEM((cap, width), F32),
            pltpu.VMEM((cap, width), F32),
            pltpu.VMEM((cap, width), F32),
            blocks(groups),
            blocks(groups),
            blocks(groups),
            blocks(nz * (np_ - 1)),
            blocks(nz * (np_ - 1)),
            blocks(nz - 1),
            blocks(nz - 1),
            blocks(DIRECT),
            blocks(DIRECT),
            dma((6,)),
            dma,
            dma((2,)),
            dma((2, nz)),
            dma,
            dma((groups,)),
            dma,
            dma((nz,)),
            dma,
            dma,
            dma,
            dma,
        ],
        compiler_params=pltpu.CompilerParams(
            collective_id=0, has_side_effects=True, vmem_limit_bytes=64000 * 1024
        ),
    )(
        bag_index,
        bag_length.T,
        emb_tables.reshape(total_rows, width),
        dense_feats,
        w_dense,
        w_pair,
        top_bias.reshape(1, units),
    )
    pooled, hidden = pl.pallas_call(
        finish,
        out_shape=results,
        in_specs=[vmem, vmem],
        out_specs=(vmem, vmem),
        compiler_params=pltpu.CompilerParams(vmem_limit_bytes=4 * 1024 * 1024),
    )(pooled, total)
    return pooled.reshape(samples, nt, width), hidden


def solution(mesh):
    nr, nc = mesh.shape["rows"], mesh.shape["cols"]
    in_specs = (
        P(("rows", "cols"), None),
        P(("rows", "cols"), None),
        P(None, ("rows", "cols"), None),
        P(("rows", "cols"), None),
        P(),
        P(),
        P(),
    )
    out_specs = (P(("rows", "cols"), None, None), P(("rows", "cols"), None))
    return jax.shard_map(
        functools.partial(shards, nr, nc),
        mesh=mesh,
        in_specs=in_specs,
        out_specs=out_specs,
        check_vma=False,
    )
```

```python
import functools

import jax
import jax.numpy as jnp
from jax import lax
from jax.experimental import pallas as pl
from jax.experimental.pallas import tpu as pltpu
from jax.sharding import PartitionSpec as P

LOGICAL = pl.DeviceIdType.LOGICAL
F32 = jnp.float32
BF16 = jnp.bfloat16
LAG = 5
CHUNKS = 8


def kernel(
    dims,
    index_hbm,
    length_hbm,
    table_hbm,
    dense_hbm,
    wd_hbm,
    wp_hbm,
    bias_hbm,
    pooled_ref,
    hidden_ref,
    index_ref,
    length_ref,
    table,
    dense_ref,
    wd,
    wp_ref,
    bias_ref,
    row_out,
    bag_out,
    bag_in,
    ids,
    rows_a,
    rows_b,
    rows_c,
    rows_d,
    core_out,
    core_in,
    keep,
    plane_out,
    plane_in,
    z_out,
    z_in,
    load_sem,
    table_sem,
    box_send,
    box_recv,
    core_send,
    core_recv,
    plane_send,
    plane_recv,
    z_send,
    z_recv,
):
    nr, nc, nx, local_rows, nt, slots_bag, cap = dims
    n = nr * nc
    ny = nc // 2
    np_ = nx * ny
    around = 2 * np_
    nz = nr // nx
    groups = nz * np_
    samples, lanes = index_ref.shape
    width = table.shape[1]
    bags = samples * nt
    total_rows = nt * local_rows
    r = lax.axis_index("rows")
    c = lax.axis_index("cols")
    z, x, y, k = r // nx, r % nx, c // 2, c % 2

    hops = sorted(
        [(dx, dy) for dx in range(nx) for dy in range(ny)],
        key=lambda h: (-min(h[0], nx - h[0]) - min(h[1], ny - h[1]), h),
    )
    back = [hops.index(((-dx) % nx, (-dy) % ny)) for dx, dy in hops]

    def plane_at(i):
        return z if i == nz - 1 else jnp.where(i < z, i, i + 1)

    def turn_at(zz):
        return jnp.where(z < zz, z, z - 1)

    planes = [plane_at(i) for i in range(nz)]
    turns = [turn_at(planes[i]) for i in range(nz - 1)] + [nz - 1]
    chips = [(((x + dx) % nx), ((y + dy) % ny)) for dx, dy in hops]

    def flat(zz, chip, kk):
        return (zz * nx + chip[0]) * nc + chip[1] * 2 + kk

    me = flat(z, (x, y), k)
    mate = flat(z, (x, y), 1 - k)
    peers = []
    for i in range(nz):
        far = z if i == nz - 1 else jnp.where(2 * z < nz, planes[nz - 2 - i], planes[i])
        turn = nz - 1 if i == nz - 1 else turn_at(far)
        for q in range(np_):
            for same in range(2):
                if (i, q, same) != (nz - 1, np_ - 1, 1):
                    d = flat(far, chips[q], k if same else 1 - k)
                    peers.append((d, turn, back[q] * 2 + same))

    load = lambda i, source, target: pltpu.make_async_copy(source, target, load_sem.at[i])
    index_copy = load(0, index_hbm, index_ref)
    length_copy = load(1, length_hbm, length_ref)
    wd_copy = load(2, wd_hbm, wd)
    dense_copy = load(3, dense_hbm, dense_ref)
    wp_copy = load(4, wp_hbm, wp_ref)
    bias_copy = load(5, bias_hbm, bias_ref)
    index_copy.start()
    length_copy.start()
    barrier = pltpu.get_barrier_semaphore()
    for d, turn, slot in peers:
        pl.semaphore_signal(barrier, inc=1, device_id=d, device_id_type=LOGICAL)
    part = total_rows // CHUNKS
    for i in range(CHUNKS):
        rows = pl.ds(i * part, part)
        pltpu.make_async_copy(table_hbm.at[rows], table.at[rows], table_sem).start()
    wd_copy.start()
    dense_copy.start()
    bias_copy.start()
    wp_copy.start()

    index_copy.wait()
    length_copy.wait()
    idx = index_ref[...]
    lane = lax.broadcasted_iota(jnp.int32, (samples, lanes), 1)
    table_of = lane // slots_bag
    length = length_ref[...].astype(F32)
    diagonal = (
        lax.broadcasted_iota(jnp.int32, (samples, samples), 0)
        == lax.broadcasted_iota(jnp.int32, (samples, samples), 1)
    )
    lengths = jnp.zeros((samples, lanes), F32)
    for t in range(nt):
        column = jnp.sum(jnp.where(diagonal, length[t : t + 1, :], 0.0), axis=1, keepdims=True)
        lengths = jnp.where(table_of == t, column, lengths)
    live = lane - table_of * slots_bag < lengths.astype(jnp.int32)
    if local_rows & (local_rows - 1) == 0:
        owner = lax.shift_right_logical(idx, jnp.full_like(idx, local_rows.bit_length() - 1))
    else:
        owner = idx // local_rows
    row = table_of * local_rows + idx - owner * local_rows
    bag = lax.broadcasted_iota(jnp.int32, (samples, lanes), 0) * nt + table_of
    owner = jnp.where(live, owner, -1)
    pieces = []
    shift = 0
    while shift == 0 or (total_rows - 1) >> shift:
        pieces.append((row // (1 << shift)) % 256)
        shift += 8
    n_row = len(pieces)
    shift = 0
    while shift == 0 or bags >> shift:
        pieces.append(((bag + 1) // (1 << shift)) % 256)
        shift += 8
    pieces = [v.astype(F32) for v in pieces]
    dev_iota = lax.broadcasted_iota(jnp.int32, (n, lanes), 0)
    before = (
        lax.broadcasted_iota(jnp.int32, (lanes, lanes), 0)
        < lax.broadcasted_iota(jnp.int32, (lanes, lanes), 1)
    )
    before = jnp.where(before, 1.0, 0.0).astype(BF16)
    hots = [
        jnp.where(owner[b : b + 1, :] == dev_iota, 1.0, 0.0).astype(F32) for b in range(samples)
    ]
    prefix = jnp.dot(
        jnp.concatenate([h.astype(BF16) for h in hots], axis=0), before, preferred_element_type=F32
    )
    base = jnp.zeros((n, 1), F32)
    box = jnp.zeros((len(pieces) * n, cap), F32)
    cap_iota = lax.broadcasted_iota(jnp.int32, (cap, lanes), 0)
    for b in range(samples):
        hot = hots[b]
        rank = jnp.sum(hot * (prefix[b * n : (b + 1) * n, :] + base), axis=0, keepdims=True)
        base = base + jnp.sum(hot, axis=1, keepdims=True)
        spot = jnp.where(rank.astype(jnp.int32) == cap_iota, 1.0, 0.0).astype(BF16)
        coded = jnp.concatenate([hot * v[b : b + 1, :] for v in pieces], axis=0).astype(BF16)
        box = box + lax.dot_general(
            coded, spot, (((1,), (1,)), ((), ())), preferred_element_type=F32
        )
    box_row = jnp.zeros((n, cap), jnp.int32)
    box_bag = jnp.full((n, cap), -1, jnp.int32)
    for i in range(len(pieces)):
        piece = box[i * n : (i + 1) * n, :].astype(jnp.int32)
        if i < n_row:
            box_row = box_row + piece * (1 << (8 * i))
        else:
            box_bag = box_bag + piece * (1 << (8 * (i - n_row)))
    if total_rows & (total_rows - 1) == 0:
        box_row = box_row & (total_rows - 1)
    else:
        box_row = jnp.clip(box_row, 0, total_rows - 1)
    for d in range(n):
        row_out[d] = box_row[d : d + 1, :]
        bag_out[d] = box_bag[d : d + 1, :]

    def copy(source, target, send, recv, d):
        return pltpu.make_async_remote_copy(
            src_ref=source,
            dst_ref=target,
            send_sem=send,
            recv_sem=recv,
            device_id=d,
            device_id_type=LOGICAL,
        )

    pl.semaphore_wait(barrier, n - 1)
    boxes = ((row_out, ids), (bag_out, bag_in))
    for i, (source, target) in enumerate(boxes):
        for d, turn, slot in peers:
            copy(
                source.at[d], target.at[turn, slot], box_send.at[i], box_recv.at[i, turn], d
            ).start()
    own_ids = load(0, row_out.at[me], ids.at[nz - 1, around - 1])
    own_ids.start()
    bag_in[nz - 1, around - 1] = bag_out[me]

    own_ids.wait()
    pltpu.make_async_copy(table_hbm, table, table_sem).wait()
    def boxes_from(i):
        some = pl.ds(0, around - 1 if i == nz - 1 else around)
        for which, (source, target) in enumerate(boxes):
            copy(
                source.at[some], target.at[i, some], box_send.at[which], box_recv.at[which, i], me
            ).wait_recv()

    bag_iota = lax.broadcasted_iota(jnp.int32, (bags, cap), 0)
    buffers = ((rows_a, rows_b), (rows_c, rows_d))

    def fetch(i, slot, target):
        for at in range(cap):
            target[at : at + 1, :] = table[pl.ds(ids[i, slot, 0, at], 1), :]

    def pool(i, slot, source):
        found = source[...]
        high = found.astype(BF16)
        low = (found - high.astype(F32)).astype(BF16)
        select = jnp.where(bag_in[i, slot] == bag_iota, 1.0, 0.0).astype(BF16)
        both = jnp.dot(select, jnp.concatenate([high, low], axis=1), preferred_element_type=F32)
        return both[:, :width] + both[:, width:]

    def core_copy(j):
        return copy(core_out.at[j], core_in.at[j], core_send, core_recv.at[j], mate)

    def forward(j):
        i, q = j // np_, j % np_
        core_copy(j).wait_recv()
        summed = core_in[j] + keep[j]
        if q == np_ - 1:
            keep[j] = summed
        else:
            at, to = i * (np_ - 1) + q, i * (np_ - 1) + back[q]
            plane_out[at] = summed
            copy(
                plane_out.at[at],
                plane_in.at[to],
                plane_send,
                plane_recv.at[i],
                flat(z, chips[q], k),
            ).start()

    def collect(i):
        some = pl.ds(i * (np_ - 1), np_ - 1)
        copy(plane_out.at[some], plane_in.at[some], plane_send, plane_recv.at[i], me).wait_recv()
        summed = keep[i * np_ + np_ - 1]
        for q in range(np_ - 1):
            summed = summed + plane_in[i * (np_ - 1) + q]
        if i < nz - 1:
            z_out[i] = summed
            copy(
                z_out.at[i], z_in.at[turns[i]], z_send, z_recv, flat(planes[i], (x, y), k)
            ).start()
        return summed

    order = list(range(groups))
    seen = set()
    for step in range(groups + LAG):
        if step < groups:
            i, q = order[step] // np_, order[step] % np_
            if i not in seen:
                seen.add(i)
                boxes_from(i)
            fetch(i, 2 * q, buffers[step % 2][0])
            fetch(i, 2 * q + 1, buffers[step % 2][1])
        if 0 < step <= groups:
            j = order[step - 1]
            i, q = j // np_, j % np_
            core_out[j] = pool(i, 2 * q, buffers[(step - 1) % 2][0])
            keep[j] = pool(i, 2 * q + 1, buffers[(step - 1) % 2][1])
            core_copy(j).start()
        if step >= LAG:
            forward(order[step - LAG])

    for i in range(nz):
        if i == nz - 1:
            wd_copy.wait()
            dense_copy.wait()
            bias_copy.wait()
            wp_copy.wait()
            dense = dense_ref[...]
            hidden_ref[...] = (
                jnp.dot(dense, wd[...], precision=lax.Precision.HIGHEST, preferred_element_type=F32)
                + bias_ref[...]
            )
        pooled = collect(i)
    if nz > 1:
        copy(z_out, z_in, z_send, z_recv, me).wait_recv()
        for i in range(nz - 1):
            pooled = pooled + z_in[i]

    pooled_ref[...] = pooled
    feats = [dense] + [pooled_ref[pl.ds(t, samples, stride=nt), :] for t in range(nt)]
    total = hidden_ref[...]
    pair = 0
    for first in range(nt + 1):
        for second in range(first + 1, nt + 1):
            dots = jnp.sum(feats[first] * feats[second], axis=-1, keepdims=True)
            total = total + dots * wp_ref[pair : pair + 1, :]
            pair += 1
    hidden_ref[...] = total

    others = pl.ds(0, n - 1)
    for which, (source, target) in enumerate(boxes):
        copy(
            source.at[others], source.at[others], box_send.at[which], box_recv.at[which, 0], me
        ).wait_send()
    copy(core_out, core_in, core_send, core_recv.at[0], me).wait_send()
    copy(plane_out, plane_in, plane_send, plane_recv.at[0], me).wait_send()
    if nz > 1:
        copy(z_out, z_in, z_send, z_recv, me).wait_send()


def finish(pooled_ref, total_ref, pooled_out, hidden_out):
    pooled_out[...] = pooled_ref[...]
    hidden_out[...] = jnp.maximum(total_ref[...], 0.0)


def shards(nr, nc, bag_index, bag_length, emb_tables, dense_feats, w_dense, w_pair, top_bias):
    samples, lanes = bag_index.shape
    nt, local_rows, width = emb_tables.shape
    n = nr * nc
    slots = samples * lanes
    cap = 2 * slots // n
    bags = samples * nt
    units = w_dense.shape[1]
    nx = 2 if nr % 2 == 0 else 1
    groups = n // 2
    nz = nr // nx
    np_ = groups // nz
    dims = (nr, nc, nx, local_rows, nt, lanes // nt, cap)
    vmem = pl.BlockSpec(memory_space=pltpu.VMEM)
    hbm = pl.BlockSpec(memory_space=pltpu.HBM)
    blocks = lambda m: pltpu.VMEM((max(m, 1), bags, width), F32)
    dma = pltpu.SemaphoreType.DMA
    results = (
        jax.ShapeDtypeStruct((bags, width), F32),
        jax.ShapeDtypeStruct((samples, units), F32),
    )
    total_rows = nt * local_rows
    pooled, total = pl.pallas_call(
        functools.partial(kernel, dims),
        out_shape=(pltpu.VMEM((bags, width), F32), pltpu.VMEM((samples, units), F32)),
        in_specs=[hbm] * 7,
        out_specs=(vmem, vmem),
        scratch_shapes=[
            pltpu.VMEM((samples, lanes), jnp.int32),
            pltpu.VMEM((nt, samples), jnp.int32),
            pltpu.VMEM((total_rows, width), F32),
            pltpu.VMEM((samples, width), F32),
            pltpu.VMEM(w_dense.shape, F32),
            pltpu.VMEM(w_pair.shape, F32),
            pltpu.VMEM((1, units), F32),
            pltpu.VMEM((n, 1, cap), jnp.int32),
            pltpu.VMEM((n, 1, cap), jnp.int32),
            pltpu.VMEM((nz, 2 * np_, 1, cap), jnp.int32),
            pltpu.SMEM((nz, 2 * np_, 1, cap), jnp.int32),
            pltpu.VMEM((cap, width), F32),
            pltpu.VMEM((cap, width), F32),
            pltpu.VMEM((cap, width), F32),
            pltpu.VMEM((cap, width), F32),
            blocks(groups),
            blocks(groups),
            blocks(groups),
            blocks(nz * (np_ - 1)),
            blocks(nz * (np_ - 1)),
            blocks(nz - 1),
            blocks(nz - 1),
            dma((6,)),
            dma,
            dma((2,)),
            dma((2, nz)),
            dma,
            dma((groups,)),
            dma,
            dma((nz,)),
            dma,
            dma,
        ],
        compiler_params=pltpu.CompilerParams(
            collective_id=0, has_side_effects=True, vmem_limit_bytes=64000 * 1024
        ),
    )(
        bag_index,
        bag_length.T,
        emb_tables.reshape(total_rows, width),
        dense_feats,
        w_dense,
        w_pair,
        top_bias.reshape(1, units),
    )
    pooled, hidden = pl.pallas_call(
        finish,
        out_shape=results,
        in_specs=[vmem, vmem],
        out_specs=(vmem, vmem),
        compiler_params=pltpu.CompilerParams(vmem_limit_bytes=4 * 1024 * 1024),
    )(pooled, total)
    return pooled.reshape(samples, nt, width), hidden


def solution(mesh):
    nr, nc = mesh.shape["rows"], mesh.shape["cols"]
    in_specs = (
        P(("rows", "cols"), None),
        P(("rows", "cols"), None),
        P(None, ("rows", "cols"), None),
        P(("rows", "cols"), None),
        P(),
        P(),
        P(),
    )
    out_specs = (P(("rows", "cols"), None, None), P(("rows", "cols"), None))
    return jax.shard_map(
        functools.partial(shards, nr, nc),
        mesh=mesh,
        in_specs=in_specs,
        out_specs=out_specs,
        check_vma=False,
    )
```

```python
import functools

import jax
import jax.numpy as jnp
from jax import lax
from jax.experimental import pallas as pl
from jax.experimental.pallas import tpu as pltpu
from jax.sharding import PartitionSpec as P

LOGICAL = pl.DeviceIdType.LOGICAL
F32 = jnp.float32
BF16 = jnp.bfloat16
LAG = 4
CHUNKS = 8


def kernel(
    dims,
    index_hbm,
    length_hbm,
    table_hbm,
    dense_hbm,
    wd_hbm,
    wp_hbm,
    bias_hbm,
    pooled_ref,
    hidden_ref,
    index_ref,
    length_ref,
    table,
    dense_ref,
    wd,
    wp_ref,
    bias_ref,
    row_out,
    bag_out,
    bag_in,
    ids,
    rows_a,
    rows_b,
    rows_c,
    rows_d,
    core_out,
    core_in,
    keep,
    plane_out,
    plane_in,
    z_out,
    z_in,
    load_sem,
    table_sem,
    box_send,
    box_recv,
    core_send,
    core_recv,
    plane_send,
    plane_recv,
    z_send,
    z_recv,
):
    nr, nc, nx, local_rows, nt, slots_bag, cap = dims
    n = nr * nc
    ny = nc // 2
    np_ = nx * ny
    around = 2 * np_
    nz = nr // nx
    groups = nz * np_
    samples, lanes = index_ref.shape
    width = table.shape[1]
    bags = samples * nt
    total_rows = nt * local_rows
    r = lax.axis_index("rows")
    c = lax.axis_index("cols")
    z, x, y, k = r // nx, r % nx, c // 2, c % 2

    hops = sorted(
        [(dx, dy) for dx in range(nx) for dy in range(ny)],
        key=lambda h: (-min(h[0], nx - h[0]) - min(h[1], ny - h[1]), h),
    )
    back = [hops.index(((-dx) % nx, (-dy) % ny)) for dx, dy in hops]

    def plane_at(i):
        return z if i == nz - 1 else jnp.where(i < z, i, i + 1)

    def turn_at(zz):
        return jnp.where(z < zz, z, z - 1)

    planes = [plane_at(i) for i in range(nz)]
    turns = [turn_at(planes[i]) for i in range(nz - 1)] + [nz - 1]
    chips = [(((x + dx) % nx), ((y + dy) % ny)) for dx, dy in hops]

    def flat(zz, chip, kk):
        return (zz * nx + chip[0]) * nc + chip[1] * 2 + kk

    me = flat(z, (x, y), k)
    mate = flat(z, (x, y), 1 - k)
    peers = []
    for i in range(nz):
        far = z if i == nz - 1 else jnp.where(2 * z < nz, planes[nz - 2 - i], planes[i])
        turn = nz - 1 if i == nz - 1 else turn_at(far)
        for q in range(np_):
            for same in range(2):
                if (i, q, same) != (nz - 1, np_ - 1, 1):
                    d = flat(far, chips[q], k if same else 1 - k)
                    peers.append((d, turn, back[q] * 2 + same))

    load = lambda i, source, target: pltpu.make_async_copy(source, target, load_sem.at[i])
    index_copy = load(0, index_hbm, index_ref)
    length_copy = load(1, length_hbm, length_ref)
    wd_copy = load(2, wd_hbm, wd)
    dense_copy = load(3, dense_hbm, dense_ref)
    wp_copy = load(4, wp_hbm, wp_ref)
    bias_copy = load(5, bias_hbm, bias_ref)
    index_copy.start()
    length_copy.start()
    barrier = pltpu.get_barrier_semaphore()
    for d, turn, slot in peers:
        pl.semaphore_signal(barrier, inc=1, device_id=d, device_id_type=LOGICAL)
    part = total_rows // CHUNKS
    for i in range(CHUNKS):
        rows = pl.ds(i * part, part)
        pltpu.make_async_copy(table_hbm.at[rows], table.at[rows], table_sem).start()
    wd_copy.start()
    dense_copy.start()
    bias_copy.start()
    wp_copy.start()

    index_copy.wait()
    length_copy.wait()
    idx = index_ref[...]
    lane = lax.broadcasted_iota(jnp.int32, (samples, lanes), 1)
    table_of = lane // slots_bag
    length = length_ref[...].astype(F32)
    diagonal = (
        lax.broadcasted_iota(jnp.int32, (samples, samples), 0)
        == lax.broadcasted_iota(jnp.int32, (samples, samples), 1)
    )
    lengths = jnp.zeros((samples, lanes), F32)
    for t in range(nt):
        column = jnp.sum(jnp.where(diagonal, length[t : t + 1, :], 0.0), axis=1, keepdims=True)
        lengths = jnp.where(table_of == t, column, lengths)
    live = lane - table_of * slots_bag < lengths.astype(jnp.int32)
    if local_rows & (local_rows - 1) == 0:
        owner = lax.shift_right_logical(idx, jnp.full_like(idx, local_rows.bit_length() - 1))
    else:
        owner = idx // local_rows
    row = table_of * local_rows + idx - owner * local_rows
    bag = lax.broadcasted_iota(jnp.int32, (samples, lanes), 0) * nt + table_of
    owner = jnp.where(live, owner, -1)
    pieces = []
    shift = 0
    while shift == 0 or (total_rows - 1) >> shift:
        pieces.append((row // (1 << shift)) % 256)
        shift += 8
    n_row = len(pieces)
    shift = 0
    while shift == 0 or bags >> shift:
        pieces.append(((bag + 1) // (1 << shift)) % 256)
        shift += 8
    pieces = [v.astype(F32) for v in pieces]
    dev_iota = lax.broadcasted_iota(jnp.int32, (n, lanes), 0)
    before = (
        lax.broadcasted_iota(jnp.int32, (lanes, lanes), 0)
        < lax.broadcasted_iota(jnp.int32, (lanes, lanes), 1)
    )
    before = jnp.where(before, 1.0, 0.0).astype(BF16)
    hots = [
        jnp.where(owner[b : b + 1, :] == dev_iota, 1.0, 0.0).astype(F32) for b in range(samples)
    ]
    prefix = jnp.dot(
        jnp.concatenate([h.astype(BF16) for h in hots], axis=0), before, preferred_element_type=F32
    )
    base = jnp.zeros((n, 1), F32)
    box = jnp.zeros((len(pieces) * n, cap), F32)
    cap_iota = lax.broadcasted_iota(jnp.int32, (cap, lanes), 0)
    for b in range(samples):
        hot = hots[b]
        rank = jnp.sum(hot * (prefix[b * n : (b + 1) * n, :] + base), axis=0, keepdims=True)
        base = base + jnp.sum(hot, axis=1, keepdims=True)
        spot = jnp.where(rank.astype(jnp.int32) == cap_iota, 1.0, 0.0).astype(BF16)
        coded = jnp.concatenate([hot * v[b : b + 1, :] for v in pieces], axis=0).astype(BF16)
        box = box + lax.dot_general(
            coded, spot, (((1,), (1,)), ((), ())), preferred_element_type=F32
        )
    box_row = jnp.zeros((n, cap), jnp.int32)
    box_bag = jnp.full((n, cap), -1, jnp.int32)
    for i in range(len(pieces)):
        piece = box[i * n : (i + 1) * n, :].astype(jnp.int32)
        if i < n_row:
            box_row = box_row + piece * (1 << (8 * i))
        else:
            box_bag = box_bag + piece * (1 << (8 * (i - n_row)))
    if total_rows & (total_rows - 1) == 0:
        box_row = box_row & (total_rows - 1)
    else:
        box_row = jnp.clip(box_row, 0, total_rows - 1)
    for d in range(n):
        row_out[d] = box_row[d : d + 1, :]
        bag_out[d] = box_bag[d : d + 1, :]

    def copy(source, target, send, recv, d):
        return pltpu.make_async_remote_copy(
            src_ref=source,
            dst_ref=target,
            send_sem=send,
            recv_sem=recv,
            device_id=d,
            device_id_type=LOGICAL,
        )

    pl.semaphore_wait(barrier, n - 1)
    boxes = ((row_out, ids), (bag_out, bag_in))
    for i, (source, target) in enumerate(boxes):
        for d, turn, slot in peers:
            copy(
                source.at[d], target.at[turn, slot], box_send.at[i], box_recv.at[i, turn], d
            ).start()
    own_ids = load(0, row_out.at[me], ids.at[nz - 1, around - 1])
    own_ids.start()
    bag_in[nz - 1, around - 1] = bag_out[me]

    own_ids.wait()
    pltpu.make_async_copy(table_hbm, table, table_sem).wait()
    def boxes_from(i):
        some = pl.ds(0, around - 1 if i == nz - 1 else around)
        for which, (source, target) in enumerate(boxes):
            copy(
                source.at[some], target.at[i, some], box_send.at[which], box_recv.at[which, i], me
            ).wait_recv()

    bag_iota = lax.broadcasted_iota(jnp.int32, (bags, cap), 0)
    buffers = ((rows_a, rows_b), (rows_c, rows_d))

    def fetch(i, slot, target):
        for at in range(cap):
            target[at : at + 1, :] = table[pl.ds(ids[i, slot, 0, at], 1), :]

    def pool(i, slot, source):
        found = source[...]
        high = found.astype(BF16)
        low = (found - high.astype(F32)).astype(BF16)
        select = jnp.where(bag_in[i, slot] == bag_iota, 1.0, 0.0).astype(BF16)
        both = jnp.dot(select, jnp.concatenate([high, low], axis=1), preferred_element_type=F32)
        return both[:, :width] + both[:, width:]

    def core_copy(j):
        return copy(core_out.at[j], core_in.at[j], core_send, core_recv.at[j], mate)

    def forward(j):
        i, q = j // np_, j % np_
        core_copy(j).wait_recv()
        summed = core_in[j] + keep[j]
        if q == np_ - 1:
            keep[j] = summed
        else:
            at, to = i * (np_ - 1) + q, i * (np_ - 1) + back[q]
            plane_out[at] = summed
            copy(
                plane_out.at[at],
                plane_in.at[to],
                plane_send,
                plane_recv.at[i],
                flat(z, chips[q], k),
            ).start()

    def collect(i):
        some = pl.ds(i * (np_ - 1), np_ - 1)
        copy(plane_out.at[some], plane_in.at[some], plane_send, plane_recv.at[i], me).wait_recv()
        summed = keep[i * np_ + np_ - 1]
        for q in range(np_ - 1):
            summed = summed + plane_in[i * (np_ - 1) + q]
        if i < nz - 1:
            z_out[i] = summed
            copy(
                z_out.at[i], z_in.at[turns[i]], z_send, z_recv, flat(planes[i], (x, y), k)
            ).start()
        return summed

    order = list(range(groups))
    seen = set()
    for step in range(groups + LAG):
        if step < groups:
            i, q = order[step] // np_, order[step] % np_
            if i not in seen:
                seen.add(i)
                boxes_from(i)
            fetch(i, 2 * q, buffers[step % 2][0])
            fetch(i, 2 * q + 1, buffers[step % 2][1])
        if 0 < step <= groups:
            j = order[step - 1]
            i, q = j // np_, j % np_
            core_out[j] = pool(i, 2 * q, buffers[(step - 1) % 2][0])
            keep[j] = pool(i, 2 * q + 1, buffers[(step - 1) % 2][1])
            core_copy(j).start()
        if step >= LAG:
            forward(order[step - LAG])

    for i in range(nz):
        if i == nz - 1:
            wd_copy.wait()
            dense_copy.wait()
            bias_copy.wait()
            wp_copy.wait()
            dense = dense_ref[...]
            hidden_ref[...] = (
                jnp.dot(dense, wd[...], precision=lax.Precision.HIGHEST, preferred_element_type=F32)
                + bias_ref[...]
            )
        pooled = collect(i)
    others = pl.ds(0, n - 1)
    for which, (source, target) in enumerate(boxes):
        copy(
            source.at[others], source.at[others], box_send.at[which], box_recv.at[which, 0], me
        ).wait_send()
    copy(core_out, core_in, core_send, core_recv.at[0], me).wait_send()
    copy(plane_out, plane_in, plane_send, plane_recv.at[0], me).wait_send()
    if nz > 1:
        copy(z_out, z_in, z_send, z_recv, me).wait_recv()
        for i in range(nz - 1):
            pooled = pooled + z_in[i]

    pooled_ref[...] = pooled
    feats = [dense] + [pooled_ref[pl.ds(t, samples, stride=nt), :] for t in range(nt)]
    total = hidden_ref[...]
    pair = 0
    for first in range(nt + 1):
        for second in range(first + 1, nt + 1):
            dots = jnp.sum(feats[first] * feats[second], axis=-1, keepdims=True)
            total = total + dots * wp_ref[pair : pair + 1, :]
            pair += 1
    hidden_ref[...] = total

    if nz > 1:
        copy(z_out, z_in, z_send, z_recv, me).wait_send()


def finish(pooled_ref, total_ref, pooled_out, hidden_out):
    pooled_out[...] = pooled_ref[...]
    hidden_out[...] = jnp.maximum(total_ref[...], 0.0)


def shards(nr, nc, bag_index, bag_length, emb_tables, dense_feats, w_dense, w_pair, top_bias):
    samples, lanes = bag_index.shape
    nt, local_rows, width = emb_tables.shape
    n = nr * nc
    slots = samples * lanes
    cap = 2 * slots // n
    bags = samples * nt
    units = w_dense.shape[1]
    nx = 2 if nr % 2 == 0 else 1
    groups = n // 2
    nz = nr // nx
    np_ = groups // nz
    dims = (nr, nc, nx, local_rows, nt, lanes // nt, cap)
    vmem = pl.BlockSpec(memory_space=pltpu.VMEM)
    hbm = pl.BlockSpec(memory_space=pltpu.HBM)
    blocks = lambda m: pltpu.VMEM((max(m, 1), bags, width), F32)
    dma = pltpu.SemaphoreType.DMA
    results = (
        jax.ShapeDtypeStruct((bags, width), F32),
        jax.ShapeDtypeStruct((samples, units), F32),
    )
    total_rows = nt * local_rows
    pooled, total = pl.pallas_call(
        functools.partial(kernel, dims),
        out_shape=(pltpu.VMEM((bags, width), F32), pltpu.VMEM((samples, units), F32)),
        in_specs=[hbm] * 7,
        out_specs=(vmem, vmem),
        scratch_shapes=[
            pltpu.VMEM((samples, lanes), jnp.int32),
            pltpu.VMEM((nt, samples), jnp.int32),
            pltpu.VMEM((total_rows, width), F32),
            pltpu.VMEM((samples, width), F32),
            pltpu.VMEM(w_dense.shape, F32),
            pltpu.VMEM(w_pair.shape, F32),
            pltpu.VMEM((1, units), F32),
            pltpu.VMEM((n, 1, cap), jnp.int32),
            pltpu.VMEM((n, 1, cap), jnp.int32),
            pltpu.VMEM((nz, 2 * np_, 1, cap), jnp.int32),
            pltpu.SMEM((nz, 2 * np_, 1, cap), jnp.int32),
            pltpu.VMEM((cap, width), F32),
            pltpu.VMEM((cap, width), F32),
            pltpu.VMEM((cap, width), F32),
            pltpu.VMEM((cap, width), F32),
            blocks(groups),
            blocks(groups),
            blocks(groups),
            blocks(nz * (np_ - 1)),
            blocks(nz * (np_ - 1)),
            blocks(nz - 1),
            blocks(nz - 1),
            dma((6,)),
            dma,
            dma((2,)),
            dma((2, nz)),
            dma,
            dma((groups,)),
            dma,
            dma((nz,)),
            dma,
            dma,
        ],
        compiler_params=pltpu.CompilerParams(
            collective_id=0, has_side_effects=True, vmem_limit_bytes=64000 * 1024
        ),
    )(
        bag_index,
        bag_length.T,
        emb_tables.reshape(total_rows, width),
        dense_feats,
        w_dense,
        w_pair,
        top_bias.reshape(1, units),
    )
    pooled, hidden = pl.pallas_call(
        finish,
        out_shape=results,
        in_specs=[vmem, vmem],
        out_specs=(vmem, vmem),
        compiler_params=pltpu.CompilerParams(vmem_limit_bytes=4 * 1024 * 1024),
    )(pooled, total)
    return pooled.reshape(samples, nt, width), hidden


def solution(mesh):
    nr, nc = mesh.shape["rows"], mesh.shape["cols"]
    in_specs = (
        P(("rows", "cols"), None),
        P(("rows", "cols"), None),
        P(None, ("rows", "cols"), None),
        P(("rows", "cols"), None),
        P(),
        P(),
        P(),
    )
    out_specs = (P(("rows", "cols"), None, None), P(("rows", "cols"), None))
    return jax.shard_map(
        functools.partial(shards, nr, nc),
        mesh=mesh,
        in_specs=in_specs,
        out_specs=out_specs,
        check_vma=False,
    )
```
